16 devices in a mesh: dp: 4 (over y, z, core), sp: 4 (over x).
Axes of the slice: x: 4, y: 2, z: 1, core: 2. Of those that a mesh axis runs over, the one named last changes fastest.
The devices are a block of a 4x4x8 slice.
Arguments:
- x: bfloat16 [8192, 7168], P(('dp', 'sp')), parts along dimension 0
- gain: bfloat16 [7168], replicated
- wq: bfloat16 [7168, 7168], replicated
- wk: bfloat16 [7168, 1024], replicated
- wv: bfloat16 [7168, 1024], replicated
- wo: bfloat16 [7168, 7168], replicated
Outputs:
- output: bfloat16 [8192, 7168], P(('dp', 'sp')), parts along dimension 0
There are 4 independent parts. The reference program is written for one: setup_inputs(seed, part) draws one part's arguments, and reference() takes and returns one part's arrays. A program takes and returns all parts, laid end to end along the dimension named above; an argument that names none is the same for every part.
All inputs are finite; a program needn't handle non-finite values.
Results may differ from the reference program's by a relative error of at most 0.012.
Values are sent between devices in bfloat16 or wider.
A program may use at most 768 MiB of HBM per device.

```python
import jax
import jax.numpy as jnp
from jax import lax

ROWS = 2048
D = 7168
HEADS = 56
KV_HEADS = 8
HEAD = 128
THETA = 10000


def setup_inputs(seed: int = 0, part: int = 0) -> dict:
    kx, kn, kq, kk, kv, ko = jax.random.split(jax.random.key(seed), 6)

    def weights(key, rows, columns):
        return jax.random.normal(key, (rows, columns), jnp.float32) * rows**-0.5

    drawn = {
        "x": jax.random.normal(jax.random.fold_in(kx, part), (ROWS, D), jnp.float32),
        "gain": 1 + 0.1 * jax.random.normal(kn, (D,), jnp.float32),
        "wq": 2 * weights(kq, D, HEADS * HEAD),
        "wk": 2 * weights(kk, D, KV_HEADS * HEAD),
        "wv": 4 * weights(kv, D, KV_HEADS * HEAD),
        "wo": weights(ko, HEADS * HEAD, D),
    }
    return {k: v.astype(jnp.bfloat16) for k, v in drawn.items()}


def normed(x, gain):
    wide = x.astype(jnp.float32)
    scale = lax.rsqrt(jnp.mean(wide * wide, -1, keepdims=True) + 1e-6)
    return (wide * scale * gain.astype(jnp.float32)).astype(jnp.bfloat16)


def turned(t, place, theta):
    half = t.shape[-1] // 2
    angle = place.astype(jnp.float32)[:, None] * theta ** (-jnp.arange(half, dtype=jnp.float32) / half)
    cos, sin = jnp.cos(angle)[:, None], jnp.sin(angle)[:, None]
    a, b = t[..., :half].astype(jnp.float32), t[..., half:].astype(jnp.float32)
    return jnp.concatenate([a * cos - b * sin, b * cos + a * sin], -1).astype(jnp.bfloat16)


def matmul(a, w):
    return jnp.dot(a, w, preferred_element_type=jnp.float32).astype(jnp.bfloat16)


def einsum(form, a, b):
    return jnp.einsum(form, a.astype(jnp.float32), b.astype(jnp.float32))


def attention(q, k, v):
    scores = einsum("tgsd,ugd->gstu", q, k) * q.shape[-1] ** -0.5
    token = jnp.arange(q.shape[0])
    scores = jnp.where(token[:, None] >= token, scores, -jnp.inf)
    weights = jax.nn.softmax(scores, -1).astype(jnp.bfloat16)
    return einsum("gstu,ugd->tgsd", weights, v).astype(jnp.bfloat16)


def reference(x, gain, wq, wk, wv, wo):
    a, place = normed(x, gain), jnp.arange(ROWS)
    q = turned(matmul(a, wq).reshape(ROWS, HEADS, HEAD), place, THETA).reshape(ROWS, KV_HEADS, -1, HEAD)
    k = turned(matmul(a, wk).reshape(ROWS, KV_HEADS, HEAD), place, THETA)
    v = matmul(a, wv).reshape(ROWS, KV_HEADS, HEAD)
    seen = attention(q, k, v).reshape(ROWS, HEADS * HEAD)
    return (x.astype(jnp.float32) + jnp.dot(seen, wo, preferred_element_type=jnp.float32)).astype(jnp.bfloat16)
```

```python
import functools

import jax
import jax.numpy as jnp
from jax import lax
from jax.experimental import pallas as pl
from jax.experimental.pallas import tpu as pltpu
from jax.sharding import PartitionSpec as P

HEAD = 128
THETA = 10000
LOG2E = 1.4426950408889634
HIDDEN = -2e30
VMEM = 60 * 2**20
TILE = 512
ANY = pl.BlockSpec(memory_space=pl.ANY)


def _dot(a, b, ca, cb):
    return lax.dot_general(a, b, (((ca,), (cb,)), ((), ())), preferred_element_type=jnp.float32)


def _turn(t, cos, sin):
    return (t * cos + pltpu.roll(t, HEAD // 2, 1) * sin).astype(jnp.bfloat16)


def _project(n, x_ref, gain_ref, cos_ref, sin_ref, wk_ref, wv_ref, wq_ref, q_ref, own_ref, p1_ref, p2_ref, p3_ref,
             a, w, kv, stage, xsem, wsem, qsem, osem, send, recv):
    rows, depth = a.shape
    nk = wk_ref.shape[1] // TILE
    tiles = 2 * nk + wq_ref.shape[1] // TILE
    slots = w.shape[0]
    me = lax.axis_index("sp")
    right, left = lax.rem(me + 1, n), lax.rem(me + n - 1, n)

    def fetch(t, go):
        def copy(ref, at):
            return pltpu.make_async_copy(ref.at[:, pl.ds(pl.multiple_of(at * TILE, TILE), TILE)], w.at[lax.rem(t, slots)], wsem.at[lax.rem(t, slots)])

        if isinstance(t, int):
            return copy(wk_ref, t).start()

        @pl.when(t < nk)
        def _():
            copy(wk_ref, t).start()

        @pl.when((t >= nk) & (t < 2 * nk))
        def _():
            copy(wv_ref, t - nk).start()

        @pl.when((t >= 2 * nk) & (t < tiles))
        def _():
            copy(wq_ref, t - 2 * nk).start()

    part = rows // 4
    loads = [pltpu.make_async_copy(x_ref.at[pl.ds(i * part, part)], a.at[pl.ds(i * part, part)], xsem.at[i]) for i in range(4)]
    loads[0].start()
    loads[1].start()
    fetch(0, True)
    loads[2].start()
    loads[3].start()
    for t in range(1, slots - 1):
        fetch(jnp.int32(t), True)

    barrier = pltpu.get_barrier_semaphore()
    for other in (left, right):
        pl.semaphore_signal(barrier, inc=1, device_id={"sp": other}, device_id_type=pl.DeviceIdType.MESH)

    for i in range(4):
        loads[i].wait()

        def norm(j, _):
            at = pl.ds(pl.multiple_of(i * part + j * 16, 16), 16)
            wide = a[at, :].astype(jnp.float32)
            scale = lax.rsqrt(jnp.mean(wide * wide, -1, keepdims=True) + 1e-6)
            a[at, :] = (wide * scale * gain_ref[...].astype(jnp.float32)).astype(jnp.bfloat16)

        lax.fori_loop(0, part // 16, norm, None)

    pl.semaphore_wait(barrier, 2)

    def remote(i, src, dst, to):
        return pltpu.make_async_remote_copy(src_ref=src, dst_ref=dst, send_sem=send.at[i], recv_sem=recv.at[i], device_id={"sp": to},
                                            device_id_type=pl.DeviceIdType.MESH)

    nt = 2 * nk
    to_right = [remote(i, kv.at[i], p1_ref.at[i], right) for i in range(nt)]
    to_left = [remote(nt + i, kv.at[i], p2_ref.at[i], left) for i in range(nt)]
    half = nk // 2
    on_right = {i: remote(2 * nt + i, p1_ref.at[i], p3_ref.at[i], right) for i in range(nt) if i % nk < half}
    on_left = {i: remote(2 * nt + i, p2_ref.at[i], p3_ref.at[i], left) for i in range(nt) if i % nk >= half}
    keep = [pltpu.make_async_copy(kv.at[i], own_ref.at[i], osem.at[i]) for i in range(nt)]

    def out(t):
        slot = lax.rem(t, 2)
        at = pl.multiple_of((t - nt) * TILE, TILE)
        return pltpu.make_async_copy(stage.at[slot], q_ref.at[:, pl.ds(at, TILE)], qsem.at[slot])

    plan = {t: [] for t in range(tiles)}
    plan[1] += [to_right[0], to_left[0]]
    plan[2] += [to_right[1], to_left[1]]
    plan[3] += [to_right[2], keep[0], keep[1]]
    plan[4] += [to_right[3], to_left[3], to_left[2], keep[2], keep[3]]
    passed = {7: ((to_right[0], on_right[0]), (to_left[1], on_left[1])), 11: ((to_right[2], on_right[2]), (to_left[3], on_left[3]))}

    def body(t, _):
        for step, copies in plan.items():
            if copies:
                @pl.when(t == step)
                def _():
                    for c in copies:
                        c.start()
        for step, pairs in passed.items():
            @pl.when(t == step)
            def _():
                for came, go in pairs:
                    came.wait_recv()
                    go.start()
        slot = lax.rem(t, slots)
        pltpu.make_async_copy(wk_ref.at[:, pl.ds(0, TILE)], w.at[slot], wsem.at[slot]).wait()
        fetch(t + slots - 1, True)

        @pl.when(t >= nt + 2)
        def _():
            out(t - 2).wait()
        res = _dot(a[...], w[slot], 1, 0).astype(jnp.bfloat16)

        @pl.when(t < nk)
        def _():
            for h in range(TILE // HEAD):
                kv[t, :, h * HEAD:(h + 1) * HEAD] = _turn(res[:, h * HEAD:(h + 1) * HEAD].astype(jnp.float32), cos_ref[...], sin_ref[...])

        @pl.when((t >= nk) & (t < nt))
        def _():
            kv[t] = res

        @pl.when(t >= nt)
        def _():
            stage[lax.rem(t, 2)] = res
            out(t).start()

    lax.fori_loop(0, tiles, body, None)
    out(tiles - 2).wait()
    out(tiles - 1).wait()
    for c in keep:
        c.wait()
    early = [to_right[0], to_right[2], to_left[1], to_left[3]]
    for c in early:
        c.wait_send()
    for c in (to_right[1], to_right[3], to_left[0], to_left[2], *on_right.values(), *on_left.values()):
        c.wait()


def project(n, x, gain, cos, sin, wk, wv, wq):
    rows, depth = x.shape
    nt = 2 * wk.shape[1] // TILE
    block = jax.ShapeDtypeStruct((nt, rows, TILE), jnp.bfloat16)
    vmem = pl.BlockSpec(memory_space=pltpu.VMEM)
    width = 2 * wk.shape[1] + wq.shape[1]
    return pl.pallas_call(
        functools.partial(_project, n),
        in_specs=[ANY, vmem, vmem, vmem, ANY, ANY, ANY],
        out_specs=[ANY] * 5,
        out_shape=[jax.ShapeDtypeStruct((rows, wq.shape[1]), jnp.bfloat16), block, block, block, block],
        scratch_shapes=[
            pltpu.VMEM((rows, depth), jnp.bfloat16),
            pltpu.VMEM((3, depth, TILE), jnp.bfloat16),
            pltpu.VMEM((nt, rows, TILE), jnp.bfloat16),
            pltpu.VMEM((2, rows, TILE), jnp.bfloat16),
            pltpu.SemaphoreType.DMA((4,)),
            pltpu.SemaphoreType.DMA((3,)),
            pltpu.SemaphoreType.DMA((2,)),
            pltpu.SemaphoreType.DMA((nt,)),
            pltpu.SemaphoreType.DMA((3 * nt,)),
            pltpu.SemaphoreType.DMA((3 * nt,)),
        ],
        compiler_params=pltpu.CompilerParams(collective_id=0, has_side_effects=True, vmem_limit_bytes=VMEM),
        cost_estimate=pl.CostEstimate(flops=2 * rows * depth * width, bytes_accessed=2 * depth * width, transcendentals=0),
        name="project",
    )(x, gain.reshape(1, -1), cos, sin, wk, wv, wq)


def _attend(q_ref, ko, vo, k1, v1, k2, v2, k3, v3, cos_ref, sin_ref, o_ref, qs, s0, s1, vt, *, g, tq, ck):
    me = lax.axis_index("sp")
    n = q_ref.shape[0]
    e = HEAD**-0.5 * LOG2E
    for h in range(g):
        qs[h] = _turn(q_ref[:, h * HEAD:(h + 1) * HEAD].astype(jnp.float32), cos_ref[...], sin_ref[...])
    ks, vs, slots = (ko, k1, k2, k3), (vo, v1, v2, v3), (s0, s1)
    strips = n // tq

    def attended(nb):
        for b in range(nb):
            vt[:HEAD, b * n:(b + 1) * n] = vs[b][0].T
        vt[HEAD:, :nb * n] = jnp.ones((8, nb * n), jnp.bfloat16)

        def chunks(s):
            size = min(ck, tq)
            own = [(0, at, size, at + size > s * tq) for at in range(0, (s + 1) * tq, size)]
            return own + [(b, at, ck, False) for b in range(1, nb) for at in range(0, n, ck)]

        def score(h, s, c, slot, off):
            b, at, size, diagonal = c
            sc = _dot(ks[b][0, at:at + size, :], qs[h, s * tq:(s + 1) * tq, :], 1, 1)
            if diagonal:
                gap = lax.broadcasted_iota(jnp.int32, sc.shape, 1) - lax.broadcasted_iota(jnp.int32, sc.shape, 0)
                sc = jnp.where(gap >= at - s * tq, sc, HIDDEN)
            slots[slot][off:off + size, :] = sc
            return sc.reshape(size // 8, 8, tq).max(axis=0)

        def unit(h, s, slot, most, following):
            now = chunks(s) if s is not None else []
            later = chunks(following[1]) if following else []
            top = most.max(axis=0, keepdims=True) if now else None
            mix = most_next = None
            off = off_next = 0
            for i in range(max(len(now), len(later))):
                if i < len(later):
                    m = score(*following, later[i], 1 - slot, off_next)
                    off_next += later[i][2]
                    most_next = m if most_next is None else jnp.maximum(most_next, m)
                if i < len(now):
                    b, at, size, _ = now[i]
                    weight = jnp.exp2((slots[slot][off:off + size, :] - top) * e).astype(jnp.bfloat16)
                    off += size
                    d = _dot(vt[:, b * n + at:b * n + at + size], weight, 1, 0)
                    mix = d if mix is None else mix + d
            if now:
                o_ref[s * tq:(s + 1) * tq, pl.ds(pl.multiple_of(h * HEAD, HEAD), HEAD)] = (mix[:HEAD] * (1 / mix[HEAD:HEAD + 1])).T.astype(o_ref.dtype)
            return most_next

        def head(h, most, last):
            for s in range(strips):
                following = (h, s + 1) if s + 1 < strips else None if last else (h + 1, 0)
                most = unit(h, s, s % 2, most, following)
            return most

        most = unit(None, None, 1, None, (0, 0))
        most = lax.fori_loop(0, g - 1, lambda h, m: head(h, m, False), most)
        head(g - 1, most, True)

    for nb in range(1, len(ks) + 1):
        pl.when(me == nb - 1)(functools.partial(attended, nb))


def attend(q, own, p1, p3, p2, cos, sin, tq=256, ck=256):
    n, width = q.shape
    per = TILE // HEAD
    kv = own.shape[0] // 2 * per
    g = width // HEAD // kv
    nk = own.shape[0] // 2
    keys = pl.BlockSpec((1, n, HEAD), lambda i: (i // per, 0, i % per))
    values = pl.BlockSpec((1, n, HEAD), lambda i: (nk + i // per, 0, i % per))
    whole = pl.BlockSpec((n, HEAD), lambda i: (0, 0))
    blocks = (own, p1, p3, p2)
    return pl.pallas_call(
        functools.partial(_attend, g=g, tq=tq, ck=ck),
        grid=(kv,),
        in_specs=[pl.BlockSpec((n, g * HEAD), lambda i: (0, i))] + [keys, values] * 4 + [whole, whole],
        out_specs=pl.BlockSpec((n, g * HEAD), lambda i: (0, i)),
        out_shape=jax.ShapeDtypeStruct((n, width), jnp.bfloat16),
        scratch_shapes=[pltpu.VMEM((g, n, HEAD), jnp.bfloat16), pltpu.VMEM((4 * n, tq), jnp.float32), pltpu.VMEM((4 * n, tq), jnp.float32),
                        pltpu.VMEM((HEAD + 8, 4 * n), jnp.bfloat16)],
        compiler_params=pltpu.CompilerParams(dimension_semantics=("arbitrary",), vmem_limit_bytes=VMEM),
        cost_estimate=pl.CostEstimate(flops=8 * n * n * width, bytes_accessed=4 * n * width, transcendentals=4 * n * n * width // HEAD),
        name="attend",
    )(q, *[t for b in blocks for t in (b, b)], cos, sin)


def tables(first, rows):
    half = HEAD // 2
    place = first + jnp.arange(rows)
    angle = place.astype(jnp.float32)[:, None] * THETA ** (-jnp.arange(half, dtype=jnp.float32) / half)
    cos, sin = jnp.cos(angle), jnp.sin(angle)
    return jnp.concatenate([cos, cos], 1), jnp.concatenate([-sin, sin], 1)


def solution(mesh):
    n = mesh.shape["sp"]

    def step(x, gain, wq, wk, wv, wo):
        rows = x.shape[0]
        cos, sin = tables(lax.axis_index("sp") * rows, rows)
        q, own, p1, p2, p3 = project(n, x, gain, cos, sin, wk, wv, wq)
        seen = attend(q, own, p1, p3, p2, cos, sin)
        y = jnp.dot(seen, wo, preferred_element_type=jnp.float32)
        return (x.astype(jnp.float32) + y).astype(jnp.bfloat16)

    tokens, whole = P(("dp", "sp"), None), P(None, None)
    return jax.shard_map(
        step,
        mesh=mesh,
        in_specs=(tokens, P(None), whole, whole, whole, whole),
        out_specs=tokens,
        check_vma=False,
    )
```

```python
import functools

import jax
import jax.numpy as jnp
from jax import lax
from jax.experimental import pallas as pl
from jax.experimental.pallas import tpu as pltpu
from jax.sharding import PartitionSpec as P

HEAD = 128
THETA = 10000
LOG2E = 1.4426950408889634
HIDDEN = -2e30
VMEM = 60 * 2**20
TILE = 512
CHUNK = 256
NORM = 64
GROUP = 4
HALF = 256
ANY = pl.BlockSpec(memory_space=pl.ANY)


def _dot(a, b, ca, cb):
    return lax.dot_general(a, b, (((ca,), (cb,)), ((), ())), preferred_element_type=jnp.float32)


def _turn(t, cos, sin):
    return (t * cos + pltpu.roll(t, HEAD // 2, 1) * sin).astype(jnp.bfloat16)


def _round(t):
    return t.astype(jnp.bfloat16).astype(jnp.float32)


def _front(n, g, x_ref, gain_ref, cos_ref, sin_ref, wk_ref, wv_ref, wq_ref, o_ref,
           cos_s, sin_s, a, w, res, own, p1, p2, p3, qb, s0, s1, xsem, wsem, osem, send, recv):
    rows, depth = a.shape
    nk = wk_ref.shape[1] // TILE
    nt = 2 * nk
    tiles = nt + wq_ref.shape[1] // TILE
    slots = w.shape[0]
    per = TILE // HEAD
    heads = qb.shape[0]
    me = lax.axis_index("sp")
    right, left = lax.rem(me + 1, n), lax.rem(me + n - 1, n)

    def piece(ref, t, at):
        slot = lax.rem(t, slots)
        return pltpu.make_async_copy(ref.at[:, pl.ds(pl.multiple_of(at * TILE, TILE), TILE)], w.at[slot], wsem.at[slot])

    part = rows // 4
    loads = [pltpu.make_async_copy(x_ref.at[pl.ds(i * part, part)], a.at[pl.ds(i * part, part)], xsem.at[i]) for i in range(4)]
    for c in loads:
        c.start()
    piece(wk_ref, 0, 0).start()

    barrier = pltpu.get_barrier_semaphore()
    for other in (left, right):
        pl.semaphore_signal(barrier, inc=1, device_id={"sp": other}, device_id_type=pl.DeviceIdType.MESH)

    weight = gain_ref[...].astype(jnp.float32).reshape(1, depth)
    cos = jnp.concatenate([cos_ref[...]] * 2, 1)
    sin = jnp.concatenate([-sin_ref[...], sin_ref[...]], 1)
    cos_s[...], sin_s[...] = cos, sin
    for i in range(4):
        loads[i].wait()

        def norm(j, _):
            at = pl.ds(pl.multiple_of(i * part + j * NORM, NORM), NORM)
            wide = a[at, :].astype(jnp.float32)
            scale = lax.rsqrt(jnp.mean(wide * wide, -1, keepdims=True) + 1e-6)
            a[at, :] = (wide * scale * weight).astype(jnp.bfloat16)

        lax.fori_loop(0, part // NORM, norm, None)
        if i == 1:
            for t in range(1, slots - 1):
                piece(wk_ref if t < nk else wv_ref, t, t % nk).start()

    pl.semaphore_wait(barrier, 2)

    def remote(i, src, dst, to):
        return pltpu.make_async_remote_copy(src_ref=src, dst_ref=dst, send_sem=send.at[i], recv_sem=recv.at[i], device_id={"sp": to},
                                            device_id_type=pl.DeviceIdType.MESH)

    to_right = [remote(i, own.at[i], p1.at[i], right) for i in range(nt)]
    to_left = [remote(nt + i, own.at[i], p2.at[i], left) for i in range(nt)]
    on_right = {i: remote(2 * nt + i, p1.at[i], p3.at[i], right) for i in (0, 2)}
    on_left = {i: remote(2 * nt + i, p2.at[i], p3.at[i], left) for i in (1, 3)}

    def at_step(t, plan):
        for step, (waits, copies) in plan.items():
            @pl.when(t == step)
            def _():
                for c in waits:
                    c.wait_recv()
                for c in copies:
                    c.start()

    def first(t, _):
        at_step(t, {1: ([], [to_right[0], to_left[0]]), 2: ([], [to_right[1], to_left[1]]), 3: ([], [to_right[2], to_left[2]])})
        piece(wk_ref, t, 0).wait()
        ahead = t + slots - 1

        @pl.when((ahead >= nk) & (ahead < nt))
        def _():
            piece(wv_ref, ahead, ahead - nk).start()

        @pl.when(ahead >= nt)
        def _():
            piece(wq_ref, ahead, ahead - nt).start()

        res[...] = _dot(a[...], w[lax.rem(t, slots)], 1, 0)

        @pl.when(t < nk)
        def _():
            for h in range(per):
                cols = slice(h * HEAD, (h + 1) * HEAD)
                own[t, :, cols] = _turn(_round(res[:, cols]), cos_s[...], sin_s[...])

        @pl.when(t >= nk)
        def _():
            own[t] = res[...].astype(jnp.bfloat16).T

    lax.fori_loop(0, nt, first, None)

    def turn(t):
        for h in range(per):
            qb[(t - nt) * per + h] = _turn(_round(res[:, h * HEAD:(h + 1) * HEAD]), cos_s[...], sin_s[...])

    def second(t, _):
        at_step(t, {4: ([], [to_left[3]]), 5: ([to_right[0]], [on_right[0]]),
                    11: ([to_right[2], to_left[1]], [on_right[2], to_right[3], on_left[1]]), 14: ([to_left[3]], [on_left[3]])})
        piece(wk_ref, t, 0).wait()

        @pl.when(t + slots - 1 < tiles)
        def _():
            piece(wq_ref, t + slots - 1, t + slots - 1 - nt).start()

        turn(jnp.maximum(t - 1, nt))
        res[...] = _dot(a[...], w[lax.rem(t, slots)], 1, 0)

    lax.fori_loop(nt, tiles, second, None)
    turn(tiles - 1)

    e = HEAD**-0.5 * LOG2E
    blocks, scores_of = (own, p1, p3, p2), (s0, s1)
    ones = jnp.ones((16, CHUNK), jnp.bfloat16)

    def save(h):
        return pltpu.make_async_copy(qb.at[h], o_ref.at[:, pl.ds(pl.multiple_of(h * HEAD, HEAD), HEAD)], osem.at[h])

    to_right[1].wait_recv()
    to_left[0].wait_recv()
    on_right[0].wait_recv()
    on_right[2].wait_recv()
    to_left[2].wait_recv()

    def attended(nb):
        chunks = [(0, at, at) for at in range(0, rows, CHUNK)] + [(b, at, 0) for b in range(1, nb) for at in range(0, rows, CHUNK)]

        def place(h):
            k = h // g
            return k // per, pl.ds(pl.multiple_of(lax.rem(k, per) * HEAD, HEAD), HEAD)

        def score(h, slot, i):
            b, at, first = chunks[i]
            tile, lanes = place(h)
            sc = _dot(blocks[b][tile, at:at + CHUNK, lanes], qb[h, first:, :], 1, 1)
            if b == 0:
                gap = lax.broadcasted_iota(jnp.int32, (CHUNK, CHUNK), 1) - lax.broadcasted_iota(jnp.int32, (CHUNK, CHUNK), 0)
                cut = jnp.where(gap >= 0, sc[:, :CHUNK], HIDDEN)
                sc = cut if first + CHUNK == rows else jnp.concatenate([cut, sc[:, CHUNK:]], 1)
            scores_of[slot][i * CHUNK:(i + 1) * CHUNK, first:] = sc
            most = sc.reshape(CHUNK // 8, 8, rows - first).max(axis=0)
            return jnp.concatenate([jnp.full((8, first), HIDDEN, jnp.float32), most], 1) if first else most

        def unit(h, slot, most, following):
            top = most.max(axis=0, keepdims=True) if h is not None else None
            most_next = None
            mix = {}
            for i, (b, at, first) in enumerate(chunks):
                if following is not None:
                    m = score(following, 1 - slot, i)
                    most_next = m if most_next is None else jnp.maximum(most_next, m)
                if h is not None:
                    tile, lanes = place(h)
                    values = jnp.concatenate([blocks[b][nk + tile, lanes, at:at + CHUNK], ones], 0)
                    weight = jnp.exp2((scores_of[slot][i * CHUNK:(i + 1) * CHUNK, first:] - top[:, first:]) * e).astype(jnp.bfloat16)
                    for c in range(first, rows, HALF):
                        d = _dot(values, weight[:, c - first:c - first + HALF], 1, 0)
                        mix[c] = mix[c] + d if c in mix else d
            if h is not None:
                for c, m in mix.items():
                    qb[h, c:c + HALF, :] = (m[:HEAD] * (1 / m[HEAD:HEAD + 1])).T.astype(o_ref.dtype)
            return most_next

        def body(i, most):
            h = GROUP * i

            @pl.when(h == heads // nk - GROUP)
            def _():
                to_right[3].wait_recv()
                on_left[1].wait_recv()
                on_left[3].wait_recv()

            @pl.when(h > 0)
            def _():
                for k in range(GROUP):
                    save(h - GROUP + k).start()

            for k in range(GROUP):
                most = unit(h + k, k % 2, most, jnp.minimum(h + k + 1, heads - 1))
            return most

        lax.fori_loop(0, heads // GROUP, body, unit(None, 1, None, 0))

    for nb in range(1, n + 1):
        pl.when(me == nb - 1)(functools.partial(attended, nb))
    for k in range(GROUP):
        save(heads - GROUP + k).start()
    lax.fori_loop(0, heads, lambda h, _: save(h).wait(), None)
    for c in (*to_right, *to_left, *on_right.values(), *on_left.values()):
        c.wait_send()


def front(n, x, gain, cos, sin, wk, wv, wq):
    rows, depth = x.shape
    nt = 2 * wk.shape[1] // TILE
    width = wq.shape[1]
    heads = width // HEAD
    vmem = pl.BlockSpec(memory_space=pltpu.VMEM)
    block = pltpu.VMEM((nt, rows, TILE), jnp.bfloat16)
    scores = pltpu.VMEM((n * rows, rows), jnp.float32)
    columns = 2 * wk.shape[1] + width
    return pl.pallas_call(
        functools.partial(_front, n, width // wk.shape[1]),
        in_specs=[ANY, vmem, vmem, vmem, ANY, ANY, ANY],
        out_specs=ANY,
        out_shape=jax.ShapeDtypeStruct((rows, width), jnp.bfloat16),
        scratch_shapes=[
            pltpu.VMEM((rows, HEAD), jnp.float32),
            pltpu.VMEM((rows, HEAD), jnp.float32),
            pltpu.VMEM((rows, depth), jnp.bfloat16),
            pltpu.VMEM((3, depth, TILE), jnp.bfloat16),
            pltpu.VMEM((rows, TILE), jnp.float32),
            block, block, block, block,
            pltpu.VMEM((heads, rows, HEAD), jnp.bfloat16),
            scores, scores,
            pltpu.SemaphoreType.DMA((4,)),
            pltpu.SemaphoreType.DMA((3,)),
            pltpu.SemaphoreType.DMA((heads,)),
            pltpu.SemaphoreType.DMA((3 * nt,)),
            pltpu.SemaphoreType.DMA((3 * nt,)),
        ],
        compiler_params=pltpu.CompilerParams(collective_id=0, has_side_effects=True, vmem_limit_bytes=VMEM),
        cost_estimate=pl.CostEstimate(flops=2 * rows * depth * columns + 8 * rows * rows * width, bytes_accessed=2 * depth * columns,
                                      transcendentals=4 * rows * rows * heads),
        name="front",
    )(x, gain, cos, sin, wk, wv, wq)


def tables(first, rows):
    half = HEAD // 2
    place = first + jnp.arange(rows)
    angle = place.astype(jnp.float32)[:, None] * THETA ** (-jnp.arange(half, dtype=jnp.float32) / half)
    return jnp.cos(angle), jnp.sin(angle)


def solution(mesh):
    n = mesh.shape["sp"]

    def step(x, gain, wq, wk, wv, wo):
        rows = x.shape[0]
        cos, sin = tables(lax.axis_index("sp") * rows, rows)
        seen = front(n, x, gain, cos, sin, wk, wv, wq)
        y = jnp.dot(seen, wo, preferred_element_type=jnp.float32)
        return (x.astype(jnp.float32) + y).astype(jnp.bfloat16)

    tokens, whole = P(("dp", "sp"), None), P(None, None)
    return jax.shard_map(
        step,
        mesh=mesh,
        in_specs=(tokens, P(None), whole, whole, whole, whole),
        out_specs=tokens,
        check_vma=False,
    )
```

```python
import functools

import jax
import jax.numpy as jnp
from jax import lax
from jax.experimental import pallas as pl
from jax.experimental.pallas import tpu as pltpu
from jax.sharding import PartitionSpec as P

HEAD = 128
THETA = 10000
LOG2E = 1.4426950408889634
HIDDEN = -2e30
VMEM = 60 * 2**20
TILE = 512
CHUNK = 256
NORM = 64
GROUP = 2
HALF = 256
ANY = pl.BlockSpec(memory_space=pl.ANY)


def _dot(a, b, ca, cb):
    return lax.dot_general(a, b, (((ca,), (cb,)), ((), ())), preferred_element_type=jnp.float32)


def _turn(t, cos, sin):
    return (t * cos + pltpu.roll(t, HEAD // 2, 1) * sin).astype(jnp.bfloat16)


def _round(t):
    return t.astype(jnp.bfloat16).astype(jnp.float32)


def _front(n, g, x_ref, gain_ref, cos_ref, sin_ref, wk_ref, wv_ref, wq_ref, o_ref,
           cos_s, sin_s, a, w, res, own, p1, p2, p3, qb, s0, s1, xsem, wsem, osem, send, recv):
    rows, depth = a.shape
    nk = wk_ref.shape[1] // TILE
    nt = 2 * nk
    tiles = nt + wq_ref.shape[1] // TILE
    slots = w.shape[0]
    per = TILE // HEAD
    heads = qb.shape[0]
    me = lax.axis_index("sp")
    right, left = lax.rem(me + 1, n), lax.rem(me + n - 1, n)

    def piece(ref, t, at):
        slot = lax.rem(t, slots)
        return pltpu.make_async_copy(ref.at[:, pl.ds(pl.multiple_of(at * TILE, TILE), TILE)], w.at[slot], wsem.at[slot])

    part = rows // 4
    loads = [pltpu.make_async_copy(x_ref.at[pl.ds(i * part, part)], a.at[pl.ds(i * part, part)], xsem.at[i]) for i in range(4)]
    for c in loads:
        c.start()
    piece(wk_ref, 0, 0).start()

    barrier = pltpu.get_barrier_semaphore()
    for other in (left, right):
        pl.semaphore_signal(barrier, inc=1, device_id={"sp": other}, device_id_type=pl.DeviceIdType.MESH)

    weight = gain_ref[...].astype(jnp.float32).reshape(1, depth)
    cos = jnp.concatenate([cos_ref[...]] * 2, 1)
    sin = jnp.concatenate([-sin_ref[...], sin_ref[...]], 1)
    cos_s[...], sin_s[...] = cos, sin
    for i in range(4):
        loads[i].wait()

        def norm(j, _):
            at = pl.ds(pl.multiple_of(i * part + j * NORM, NORM), NORM)
            wide = a[at, :].astype(jnp.float32)
            scale = lax.rsqrt(jnp.mean(wide * wide, -1, keepdims=True) + 1e-6)
            a[at, :] = (wide * scale * weight).astype(jnp.bfloat16)

        lax.fori_loop(0, part // NORM, norm, None)
        if i == 1:
            for t in range(1, slots - 1):
                piece(wk_ref if t < nk else wv_ref, t, t % nk).start()

    pl.semaphore_wait(barrier, 2)

    def remote(i, src, dst, to):
        return pltpu.make_async_remote_copy(src_ref=src, dst_ref=dst, send_sem=send.at[i], recv_sem=recv.at[i], device_id={"sp": to},
                                            device_id_type=pl.DeviceIdType.MESH)

    to_right = [remote(i, own.at[i], p1.at[i], right) for i in range(nt)]
    to_left = [remote(nt + i, own.at[i], p2.at[i], left) for i in range(nt)]
    on_right = {i: remote(2 * nt + i, p1.at[i], p3.at[i], right) for i in (0, 2)}
    on_left = {i: remote(2 * nt + i, p2.at[i], p3.at[i], left) for i in (1, 3)}

    def at_step(t, plan):
        for step, (waits, copies) in plan.items():
            @pl.when(t == step)
            def _():
                for c in waits:
                    c.wait_recv()
                for c in copies:
                    c.start()

    def first(t, _):
        at_step(t, {1: ([], [to_right[0], to_left[0]]), 2: ([], [to_right[1], to_left[1]]), 3: ([], [to_right[2], to_left[2]])})
        piece(wk_ref, t, 0).wait()
        ahead = t + slots - 1

        @pl.when((ahead >= nk) & (ahead < nt))
        def _():
            piece(wv_ref, ahead, ahead - nk).start()

        @pl.when(ahead >= nt)
        def _():
            piece(wq_ref, ahead, ahead - nt).start()

        res[...] = _dot(a[...], w[lax.rem(t, slots)], 1, 0)

        @pl.when(t < nk)
        def _():
            for h in range(per):
                cols = slice(h * HEAD, (h + 1) * HEAD)
                own[t, :, cols] = _turn(_round(res[:, cols]), cos_s[...], sin_s[...])

        @pl.when(t >= nk)
        def _():
            own[t] = res[...].astype(jnp.bfloat16).T

    lax.fori_loop(0, nt, first, None)

    def turn(t):
        for h in range(per):
            qb[(t - nt) * per + h] = _turn(_round(res[:, h * HEAD:(h + 1) * HEAD]), cos_s[...], sin_s[...])

    def second(t, _):
        at_step(t, {4: ([], [to_left[3]]), 5: ([to_right[0]], [on_right[0]]),
                    11: ([to_right[2], to_left[1]], [on_right[2], to_right[3], on_left[1]]), 14: ([to_left[3]], [on_left[3]])})
        piece(wk_ref, t, 0).wait()

        @pl.when(t + slots - 1 < tiles)
        def _():
            piece(wq_ref, t + slots - 1, t + slots - 1 - nt).start()

        turn(jnp.maximum(t - 1, nt))
        res[...] = _dot(a[...], w[lax.rem(t, slots)], 1, 0)

    lax.fori_loop(nt, tiles, second, None)
    turn(tiles - 1)

    e = HEAD**-0.5 * LOG2E
    blocks, scores_of = (own, p1, p3, p2), (s0, s1)
    ones = jnp.ones((16, CHUNK), jnp.bfloat16)

    def save(h):
        return pltpu.make_async_copy(qb.at[h], o_ref.at[:, pl.ds(pl.multiple_of(h * HEAD, HEAD), HEAD)], osem.at[h])

    to_right[1].wait_recv()
    to_left[0].wait_recv()
    on_right[0].wait_recv()
    on_right[2].wait_recv()
    to_left[2].wait_recv()

    def attended(nb):
        chunks = [(0, at, at) for at in range(0, rows, CHUNK)] + [(b, at, 0) for b in range(1, nb) for at in range(0, rows, CHUNK)]

        def place(h):
            k = h // g
            return k // per, pl.ds(pl.multiple_of(lax.rem(k, per) * HEAD, HEAD), HEAD)

        def score(h, slot, i):
            b, at, first = chunks[i]
            tile, lanes = place(h)
            sc = _dot(blocks[b][tile, at:at + CHUNK, lanes], qb[h, first:, :], 1, 1)
            if b == 0:
                gap = lax.broadcasted_iota(jnp.int32, (CHUNK, CHUNK), 1) - lax.broadcasted_iota(jnp.int32, (CHUNK, CHUNK), 0)
                cut = jnp.where(gap >= 0, sc[:, :CHUNK], HIDDEN)
                sc = cut if first + CHUNK == rows else jnp.concatenate([cut, sc[:, CHUNK:]], 1)
            scores_of[slot][i * CHUNK:(i + 1) * CHUNK, first:] = sc
            most = sc.reshape(CHUNK // 8, 8, rows - first).max(axis=0)
            return jnp.concatenate([jnp.full((8, first), HIDDEN, jnp.float32), most], 1) if first else most

        def unit(h, slot, most, following):
            top = most.max(axis=0, keepdims=True) if h is not None else None
            most_next = None
            mix = {}
            for i, (b, at, first) in enumerate(chunks):
                if following is not None:
                    m = score(following, 1 - slot, i)
                    most_next = m if most_next is None else jnp.maximum(most_next, m)
                if h is not None:
                    tile, lanes = place(h)
                    values = jnp.concatenate([blocks[b][nk + tile, lanes, at:at + CHUNK], ones], 0)
                    weight = jnp.exp2((scores_of[slot][i * CHUNK:(i + 1) * CHUNK, first:] - top[:, first:]) * e).astype(jnp.bfloat16)
                    for c in range(first, rows, HALF):
                        d = _dot(values, weight[:, c - first:c - first + HALF], 1, 0)
                        mix[c] = mix[c] + d if c in mix else d
            if h is not None:
                for c, m in mix.items():
                    qb[h, c:c + HALF, :] = (m[:HEAD] * (1 / m[HEAD:HEAD + 1])).astype(o_ref.dtype).T
            return most_next

        def body(i, most):
            h = GROUP * i

            @pl.when(h == heads // nk - GROUP)
            def _():
                to_right[3].wait_recv()
                on_left[1].wait_recv()
                on_left[3].wait_recv()

            @pl.when(h > 0)
            def _():
                for k in range(GROUP):
                    save(h - GROUP + k).start()

            for k in range(GROUP):
                most = unit(h + k, k % 2, most, jnp.minimum(h + k + 1, heads - 1))
            return most

        lax.fori_loop(0, heads // GROUP, body, unit(None, 1, None, 0))

    for nb in range(1, n + 1):
        pl.when(me == nb - 1)(functools.partial(attended, nb))
    for k in range(GROUP):
        save(heads - GROUP + k).start()
    lax.fori_loop(0, heads, lambda h, _: save(h).wait(), None)
    for c in (*to_right, *to_left, *on_right.values(), *on_left.values()):
        c.wait_send()


def front(n, x, gain, cos, sin, wk, wv, wq):
    rows, depth = x.shape
    nt = 2 * wk.shape[1] // TILE
    width = wq.shape[1]
    heads = width // HEAD
    vmem = pl.BlockSpec(memory_space=pltpu.VMEM)
    block = pltpu.VMEM((nt, rows, TILE), jnp.bfloat16)
    scores = pltpu.VMEM((n * rows, rows), jnp.float32)
    columns = 2 * wk.shape[1] + width
    return pl.pallas_call(
        functools.partial(_front, n, width // wk.shape[1]),
        in_specs=[ANY, vmem, vmem, vmem, ANY, ANY, ANY],
        out_specs=ANY,
        out_shape=jax.ShapeDtypeStruct((rows, width), jnp.bfloat16),
        scratch_shapes=[
            pltpu.VMEM((rows, HEAD), jnp.float32),
            pltpu.VMEM((rows, HEAD), jnp.float32),
            pltpu.VMEM((rows, depth), jnp.bfloat16),
            pltpu.VMEM((3, depth, TILE), jnp.bfloat16),
            pltpu.VMEM((rows, TILE), jnp.float32),
            block, block, block, block,
            pltpu.VMEM((heads, rows, HEAD), jnp.bfloat16),
            scores, scores,
            pltpu.SemaphoreType.DMA((4,)),
            pltpu.SemaphoreType.DMA((3,)),
            pltpu.SemaphoreType.DMA((heads,)),
            pltpu.SemaphoreType.DMA((3 * nt,)),
            pltpu.SemaphoreType.DMA((3 * nt,)),
        ],
        compiler_params=pltpu.CompilerParams(collective_id=0, has_side_effects=True, vmem_limit_bytes=VMEM),
        cost_estimate=pl.CostEstimate(flops=2 * rows * depth * columns + 8 * rows * rows * width, bytes_accessed=2 * depth * columns,
                                      transcendentals=4 * rows * rows * heads),
        name="front",
    )(x, gain, cos, sin, wk, wv, wq)


def _back(s_ref, x_ref, w_ref, y_ref, a, w, xs, ys, asem, wsem, xsem, ysem):
    slots = w.shape[0]
    tiles = w_ref.shape[1] // TILE

    def columns(t):
        return pl.ds(pl.multiple_of(t * TILE, TILE), TILE)

    def weight(t):
        slot = lax.rem(t, slots)
        return pltpu.make_async_copy(w_ref.at[:, columns(t)], w.at[slot], wsem.at[slot])

    def given(t):
        slot = lax.rem(t, 2)
        return pltpu.make_async_copy(x_ref.at[:, columns(t)], xs.at[slot], xsem.at[slot])

    def result(t):
        slot = lax.rem(t, 2)
        return pltpu.make_async_copy(ys.at[slot], y_ref.at[:, columns(t)], ysem.at[slot])

    whole = pltpu.make_async_copy(s_ref, a, asem)
    whole.start()
    weight(0).start()
    given(0).start()
    for t in range(1, slots - 1):
        weight(t).start()
    whole.wait()

    def body(t, _):
        weight(t).wait()
        given(t).wait()

        @pl.when(t + slots - 1 < tiles)
        def _():
            weight(t + slots - 1).start()

        @pl.when(t + 1 < tiles)
        def _():
            given(t + 1).start()

        @pl.when(t >= 2)
        def _():
            result(t - 2).wait()

        slot = lax.rem(t, 2)
        ys[slot] = (_dot(a[...], w[lax.rem(t, slots)], 1, 0) + xs[slot].astype(jnp.float32)).astype(jnp.bfloat16)
        result(t).start()

    lax.fori_loop(0, tiles, body, None)
    result(tiles - 2).wait()
    result(tiles - 1).wait()


def back(seen, x, wo):
    rows, depth = seen.shape
    return pl.pallas_call(
        _back,
        in_specs=[ANY] * 3,
        out_specs=ANY,
        out_shape=jax.ShapeDtypeStruct(x.shape, x.dtype),
        scratch_shapes=[
            pltpu.VMEM((rows, depth), jnp.bfloat16),
            pltpu.VMEM((3, depth, TILE), jnp.bfloat16),
            pltpu.VMEM((2, rows, TILE), jnp.bfloat16),
            pltpu.VMEM((2, rows, TILE), jnp.bfloat16),
            pltpu.SemaphoreType.DMA,
            pltpu.SemaphoreType.DMA((3,)),
            pltpu.SemaphoreType.DMA((2,)),
            pltpu.SemaphoreType.DMA((2,)),
        ],
        compiler_params=pltpu.CompilerParams(vmem_limit_bytes=VMEM),
        cost_estimate=pl.CostEstimate(flops=2 * rows * depth * x.shape[1], bytes_accessed=2 * depth * x.shape[1], transcendentals=0),
        name="back",
    )(seen, x, wo)


def tables(first, rows):
    half = HEAD // 2
    place = first + jnp.arange(rows)
    angle = place.astype(jnp.float32)[:, None] * THETA ** (-jnp.arange(half, dtype=jnp.float32) / half)
    return jnp.cos(angle), jnp.sin(angle)


def solution(mesh):
    n = mesh.shape["sp"]

    def step(x, gain, wq, wk, wv, wo):
        rows = x.shape[0]
        cos, sin = tables(lax.axis_index("sp") * rows, rows)
        seen = front(n, x, gain, cos, sin, wk, wv, wq)
        return back(seen, x, wo)

    tokens, whole = P(("dp", "sp"), None), P(None, None)
    return jax.shard_map(
        step,
        mesh=mesh,
        in_specs=(tokens, P(None), whole, whole, whole, whole),
        out_specs=tokens,
        check_vma=False,
    )
```
